32 devices in a mesh: member: 2 (over x), tile: 16 (over z, y, core).
Axes of the slice: x: 2, y: 2, z: 4, core: 2. Of those that a mesh axis runs over, the one named last changes fastest.
Arguments:
- pressure: float32 [64, 128, 512], P('member', 'tile'), parts along dimension 0, may hold values from -1.5 to 1
- conductivity: float32 [64, 128, 512], P('member', 'tile'), parts along dimension 0, may hold values from 0.5 to 2
- soil_class: int32 [64, 128, 512], P('member', 'tile'), parts along dimension 0, may hold values from 0 to 11
- vg_alpha: float32 [12], replicated, may hold values from 0.3 to 2
- vg_shape: float32 [12], replicated, may hold values from 1.3 to 2.6
- bed: float32 [512, 256], P('tile', 'member'), parts along dimension 1, may hold values from -4 to 4
- flow_code: int32 [512, 256], P('tile', 'member'), parts along dimension 1, may hold values from 0 to 7
- surface_soil: int32 [512, 256], P('tile', 'member'), parts along dimension 1, may hold values from 0 to 11
- cover_class: int32 [512, 256], P('tile', 'member'), parts along dimension 1, may hold values from 0 to 16
- ponding: int32 [512, 256], P('tile', 'member'), parts along dimension 1, may hold values 0 or 1
- conveyance: float32 [17], replicated, may hold values from 0.3 to 3
- erodibility: float32 [12], replicated, may hold values from 0.1 to 1
Outputs:
- head_out: float32 [64, 128, 512], P('member', 'tile'), parts along dimension 0
- bed_out: float32 [512, 256], P('tile', 'member'), parts along dimension 1
The draws below stay inside these ranges and needn't reach their ends.
There are 2 independent parts, one for each index of `member`. The reference program is written for one: setup_inputs(seed, part) draws one part's arguments, and reference() takes and returns one part's arrays. A program takes and returns all parts, laid end to end along the dimension named above; an argument that names none is the same for every part. Nothing has to cross between parts.
All inputs are finite; a program needn't handle non-finite values. No bound on the sum of `ponding` on one device may be relied on, other than what follows from the above.
Results may differ from the reference program's by a relative error of at most 0.00035.
Values sent between devices are 32-bit elements; how exact they have to be, the bound alone decides.
A program may use at most 128 MiB of HBM per device.

```python
import math
import jax
import jax.numpy as jnp

LAYERS = 32
STEPS = 4
CLASSES = 12
COVERS = 17
NX = 128
NY = 512


def touch_ends(values, stream_key, smallest, high):
    spot = [jax.random.randint(jax.random.fold_in(stream_key, axis), (), 0, length) for axis, length in enumerate(values.shape)]
    widest = values.shape.index(max(values.shape))
    next_to = spot[:widest] + [(spot[widest] + 1) % values.shape[widest]] + spot[widest + 1:]
    return values.at[tuple(spot)].set(smallest).at[tuple(next_to)].set(high)


def levels(key, extent, shards, smallest, high):
    gain, own = 1.0, jax.random.fold_in(key, 6)
    for position, parts in shards:
        heights = jnp.exp(jax.random.uniform(jax.random.fold_in(own, position), (parts,), jnp.float32, smallest / len(shards), high / len(shards)))
        gain = gain * jnp.repeat(heights, extent[position] // parts).reshape([-1 if axis == position else 1 for axis in range(len(extent))])
    return gain


def bell_draw(key, extent, scale, limit, split=(), kind=jnp.bfloat16):
    drawn = scale * jax.random.normal(key, extent, jnp.float32)
    if split:
        drawn = drawn * levels(key, extent, split, -0.22, 0.18)
    return jnp.clip(drawn, -limit, limit).astype(kind)


def setup_inputs(seed: int = 0, part: int = 0) -> dict:
    streams_of = jax.random.split(jax.random.key(seed), 13)
    own_keys = jax.random.split(jax.random.fold_in(streams_of[12], part), 13)
    return {
        "pressure": jnp.clip(-1.5 + 2.5 * jax.random.uniform(own_keys[0], (LAYERS, NX, NY), jnp.float32) ** levels(own_keys[0], (LAYERS, NX, NY), ((1, 16),), -0.2, 0.2), -1.5, 1.0),
        "conductivity": jnp.clip(jnp.exp(math.log(2.0) - 1.3862944 * jax.random.uniform(own_keys[1], (LAYERS, NX, NY), jnp.float32) ** levels(own_keys[1], (LAYERS, NX, NY), ((1, 16),), -0.2, 0.2)), 0.5, 2.0),
        "soil_class": touch_ends(jax.random.randint(own_keys[2], (LAYERS, NX, NY), 0, CLASSES), jax.random.fold_in(own_keys[2], 1), 0, CLASSES - 1).astype(jnp.int32),
        "vg_alpha": jnp.clip(jnp.exp(jax.random.uniform(streams_of[3], (CLASSES,), jnp.float32, math.log(0.3), math.log(2.0))), 0.3, 2.0),
        "vg_shape": jnp.clip(jax.random.uniform(streams_of[4], (CLASSES,), jnp.float32, 1.3, 2.6), 1.3, 2.6),
        "bed": bell_draw(own_keys[5], (NY, NX), 1.0, 4.0, ((0, 16),), jnp.float32),
        "flow_code": touch_ends(jax.random.randint(own_keys[6], (NY, NX), 0, 8), jax.random.fold_in(own_keys[6], 1), 0, 7).astype(jnp.int32),
        "surface_soil": touch_ends(jax.random.randint(own_keys[7], (NY, NX), 0, CLASSES), jax.random.fold_in(own_keys[7], 1), 0, CLASSES - 1).astype(jnp.int32),
        "cover_class": touch_ends(jax.random.randint(own_keys[8], (NY, NX), 0, COVERS), jax.random.fold_in(own_keys[8], 1), 0, COVERS - 1).astype(jnp.int32),
        "ponding": touch_ends((jax.random.randint(own_keys[9], (NY, NX), 0, 4) < 1).astype(jnp.int32), jax.random.fold_in(own_keys[9], 1), 0, 1),
        "conveyance": jnp.clip(jnp.exp(jax.random.uniform(streams_of[10], (COVERS,), jnp.float32, math.log(0.3), math.log(3.0))), 0.3, 3.0),
        "erodibility": jnp.clip(jnp.exp(jax.random.uniform(streams_of[11], (CLASSES,), jnp.float32, math.log(0.1), math.log(1.0))), 0.1, 1.0),
    }


RELAX_STEP = 0.08
CAPACITY = 2.0
MIN_SLOPE = 0.01
BED_RATE = 2.0
SHIFT_X = (1, 1, 0, -1, -1, -1, 0, 1)
SHIFT_Y = (0, 1, 1, 1, 0, -1, -1, -1)

def retention(head, alpha_field, shape_field):
    exponent = 1.0 - 1.0 / shape_field
    suction = jnp.maximum(-head, 0.0)
    saturation = (1.0 + (alpha_field * suction) ** shape_field) ** (-exponent)
    inner = jnp.maximum(1.0 - saturation ** (1.0 / exponent), 0.0)
    permeab = jnp.sqrt(saturation) * (1.0 - inner ** exponent) ** 2
    return (saturation, permeab)

def relax(wide_head, wide_ks, wide_alpha, wide_shape):
    saturation, permeab = retention(wide_head, wide_alpha, wide_shape)
    conduct = wide_ks * permeab
    layers = wide_head.shape[0]
    height = wide_head - jnp.arange(layers, dtype=wide_head.dtype)[:, None, None]
    centre_k = conduct[:, 1:-1]
    centre_h = height[:, 1:-1]
    flow = 0.5 * (centre_k + conduct[:, 2:]) * (height[:, 2:] - centre_h)
    flow = flow + 0.5 * (centre_k + conduct[:, :-2]) * (height[:, :-2] - centre_h)
    side_k = jnp.pad(centre_k, ((0, 0), (0, 0), (1, 1)), mode='edge')
    side_h = jnp.pad(centre_h, ((0, 0), (0, 0), (1, 1)), mode='edge')
    flow = flow + 0.5 * (centre_k + side_k[:, :, 2:]) * (side_h[:, :, 2:] - centre_h)
    flow = flow + 0.5 * (centre_k + side_k[:, :, :-2]) * (side_h[:, :, :-2] - centre_h)
    vertical = 0.5 * (centre_k[:-1] + centre_k[1:]) * (centre_h[1:] - centre_h[:-1])
    zero_plane = jnp.zeros_like(vertical[:1])
    flow = flow + jnp.concatenate([vertical, zero_plane], 0) - jnp.concatenate([zero_plane, vertical], 0)
    drain = jnp.concatenate([jnp.zeros_like(centre_k[:-1]), centre_k[-1:]], 0)
    flow = flow - drain
    return wide_head[:, 1:-1] + RELAX_STEP * flow / (1.0 + CAPACITY * (1.0 - saturation[:, 1:-1]))

def surface_step(wide_bed, wide_depth, wide_coef, wide_erode, wide_code, rows, columns, flipped):

    def window(field, first, second):
        return field[1 + first:rows + 3 + first, 1 + second:columns + 3 + second]

    def source(field, first, second):
        return field[1 - first:rows + 1 - first, 1 - second:columns + 1 - second]
    shifts = []
    for course in range(8):
        if flipped:
            shifts.append((SHIFT_X[course], SHIFT_Y[course]))
        else:
            shifts.append((SHIFT_Y[course], SHIFT_X[course]))
    centre = window(wide_bed, 0, 0)
    codes = window(wide_code, 0, 0)
    slope = jnp.full_like(centre, MIN_SLOPE)
    for course in range(8):
        first, second = shifts[course]
        distance = math.sqrt(first * first + second * second)
        drop = jnp.maximum(centre - window(wide_bed, first, second), 0.0) / distance
        slope = slope + jnp.where(codes == course, drop, 0.0)
    depth = window(wide_depth, 0, 0)
    root_slope = jnp.sqrt(slope)
    drive = window(wide_coef, 0, 0) * root_slope * depth ** (2.0 / 3.0)
    outflow = depth * drive / (1.0 + drive)
    sediment = window(wide_erode, 0, 0) * outflow * root_slope
    inflow = jnp.zeros_like(outflow[1:rows + 1, 1:columns + 1])
    sed_in = jnp.zeros_like(inflow)
    for course in range(8):
        first, second = shifts[course]
        chosen = source(codes, first, second) == course
        inflow = inflow + jnp.where(chosen, source(outflow, first, second), 0.0)
        sed_in = sed_in + jnp.where(chosen, source(sediment, first, second), 0.0)
    change = inflow - outflow[1:rows + 1, 1:columns + 1]
    bed_change = BED_RATE * (sed_in - sediment[1:rows + 1, 1:columns + 1])
    return (change, bed_change)

def reference(pressure, conductivity, soil_class, vg_alpha, vg_shape, bed, flow_code, surface_soil, cover_class, ponding, conveyance, erodibility):
    alpha_field = vg_alpha[soil_class]
    shape_field = vg_shape[soil_class]
    coef = conveyance[cover_class] * (1.0 - ponding.astype(jnp.float32))
    erode = erodibility[surface_soil]
    codes = flow_code.astype(jnp.float32)
    xpad = ((0, 0), (1, 1), (0, 0))
    ks_wide = jnp.pad(conductivity, xpad, mode='edge')
    alpha_wide = jnp.pad(alpha_field, xpad, mode='edge')
    shape_wide = jnp.pad(shape_field, xpad, mode='edge')
    coef_wide = jnp.pad(coef, 2)
    erode_wide = jnp.pad(erode, 2)
    code_wide = jnp.pad(codes, 2)
    head = pressure
    level = bed
    for section_index in range(STEPS):
        for sweep_index in range(2):
            head = relax(jnp.pad(head, xpad, mode='edge'), ks_wide, alpha_wide, shape_wide)
        depth = jnp.maximum(head[0].T, 0.0)
        change, bed_change = surface_step(jnp.pad(level, 2), jnp.pad(depth, 2), coef_wide, erode_wide, code_wide, NY, NX, False)
        head = head.at[0].add(change.T)
        level = level + bed_change
    return (head, level)
```

```python
import functools
import math

import jax
import jax.numpy as jnp
from jax import lax
from jax.experimental import pallas as pl
from jax.experimental.pallas import tpu as pltpu
from jax.sharding import PartitionSpec as P

STEPS = 4
RELAX_STEP = 0.08
CAPACITY = 2.0
MIN_SLOPE = 0.01
BED_RATE = 2.0
SHIFT_X = (1, 1, 0, -1, -1, -1, 0, 1)
SHIFT_Y = (0, 1, 1, 1, 0, -1, -1, -1)
TINY = 1.2e-38
LANES = 128
HEAD_A, HEAD_B, DEPTH, LEVEL, SOIL_K, SOIL_C = range(6)


def table_pick(classes, table, entries):
    picked = jnp.full(classes.shape, table(0), jnp.float32)
    for entry in range(1, entries):
        picked = jnp.where(classes == entry, table(entry), picked)
    return picked


def turn(values, shift, axis):
    shift = shift % values.shape[axis]
    return values if shift == 0 else pltpu.roll(values, shift, axis)


def kernel(
    count,
    head_in,
    ks_in,
    class_in,
    alpha_t,
    shape_t,
    bed_in,
    code_in,
    soil_in,
    cover_in,
    pond_in,
    convey_t,
    erod_t,
    head_out,
    bed_out,
    head_a,
    head_b,
    half_k,
    gain,
    ks,
    alpha,
    shape,
    half_m,
    levels,
    depths,
    maps,
    classes,
    packed,
    gathered,
    final_src,
    final_dst,
    turned,
    send_sem,
    recv_sem,
    spread_send,
    spread_recv,
    final_send,
    final_recv,
):
    rows, layers, columns = head_in.shape
    strip = bed_in.shape[0]
    width = bed_in.shape[1]
    per = LANES // strip
    groups = columns // LANES
    me = lax.axis_index("tile")
    has_left = me > 0
    has_right = me < count - 1
    low = 1 - (me + count - 1) // count
    high = rows + (2 * count - 2 - me) // count

    def at(tile):
        return {"tile": tile}

    def to_left(kind, src, dst):
        return pltpu.make_async_remote_copy(
            src_ref=src,
            dst_ref=dst,
            send_sem=send_sem.at[kind, 0],
            recv_sem=recv_sem.at[kind, 1],
            device_id=at(me - 1),
            device_id_type=pl.DeviceIdType.MESH,
        )

    def to_right(kind, src, dst):
        return pltpu.make_async_remote_copy(
            src_ref=src,
            dst_ref=dst,
            send_sem=send_sem.at[kind, 1],
            recv_sem=recv_sem.at[kind, 0],
            device_id=at(me + 1),
            device_id_type=pl.DeviceIdType.MESH,
        )

    def push(kind, first, last, low_halo, high_halo):
        @pl.when(has_left)
        def _():
            to_left(kind, first, high_halo).start()

        @pl.when(has_right)
        def _():
            to_right(kind, last, low_halo).start()

    def await_recv(kind, low_halo, high_halo):
        @pl.when(has_left)
        def _():
            to_right(kind, low_halo, low_halo).wait_recv()

        @pl.when(has_right)
        def _():
            to_left(kind, high_halo, high_halo).wait_recv()

    def await_send(kind, first, last):
        @pl.when(has_left)
        def _():
            to_left(kind, first, first).wait_send()

        @pl.when(has_right)
        def _():
            to_right(kind, last, last).wait_send()

    levels[...] = jnp.zeros_like(levels)
    depths[...] = jnp.zeros_like(depths)

    coef_y = table_pick(cover_in[...], lambda i: convey_t[i], convey_t.shape[0]) * (
        1.0 - pond_in[...].astype(jnp.float32)
    )
    erode_y = table_pick(soil_in[...], lambda i: erod_t[i], erod_t.shape[0])
    stacked = jnp.concatenate(
        [coef_y, erode_y, code_in[...].astype(jnp.float32), bed_in[...]], axis=0
    )
    packed[0:rows] = jnp.zeros((rows, LANES), jnp.float32)
    packed[rows + width : 2 * rows + width] = jnp.zeros((rows, LANES), jnp.float32)
    for block in range(width // LANES):
        packed[rows + block * LANES : rows + (block + 1) * LANES] = jnp.transpose(
            stacked[:, block * LANES : (block + 1) * LANES]
        )

    barrier = pltpu.get_barrier_semaphore()
    for away in range(1, count):
        pl.semaphore_signal(
            barrier,
            inc=1,
            device_id=at(lax.rem(me + away, count)),
            device_id_type=pl.DeviceIdType.MESH,
        )
    pl.semaphore_wait(barrier, count - 1)

    last_row = rows + 1
    push(SOIL_C, class_in.at[0], class_in.at[rows - 1], classes.at[0], classes.at[1])
    push(SOIL_K, ks_in.at[0], ks_in.at[rows - 1], ks.at[0], ks.at[last_row])
    push(HEAD_A, head_in.at[0], head_in.at[rows - 1], head_a.at[0], head_a.at[last_row])

    def spread(away):
        peer = lax.rem(me + away, count)
        return pltpu.make_async_remote_copy(
            src_ref=packed.at[pl.ds(pl.multiple_of(peer * rows, rows), 3 * rows)],
            dst_ref=gathered.at[me],
            send_sem=spread_send.at[away],
            recv_sem=spread_recv.at[away],
            device_id=at(peer),
            device_id_type=pl.DeviceIdType.MESH,
        )

    for away in range(1, count):
        spread(away).start()
    gathered[me] = packed[pl.ds(pl.multiple_of(me * rows, rows), 3 * rows)]

    def soil_row(row, found):
        alpha[row] = table_pick(found, lambda i: alpha_t[i], alpha_t.shape[0])
        bend = table_pick(found, lambda i: shape_t[i], shape_t.shape[0])
        shape[row] = bend
        half_m[row] = 0.5 / bend - 0.5

    @pl.loop(0, rows)
    def _(row):
        soil_row(row + 1, class_in[row])
        ks[row + 1] = 0.5 * ks_in[row]
        head_a[row + 1] = head_in[row]

    def conduct_row(head, row, keep):
        bend = shape[row]
        log_a = lax.log2(alpha[row] * jnp.maximum(-head[row], TINY))
        log_w = lax.log2(1.0 + lax.exp2(bend * log_a))
        root = lax.exp2(half_m[row] * log_w)
        full = root * root
        inner = 1.0 - lax.exp2((bend - 1.0) * log_a) * full
        half_k[row] = ks[row] * root * (inner * inner)
        if keep:
            gain[row] = RELAX_STEP / (1.0 + CAPACITY * (1.0 - full))

    layer = lax.broadcasted_iota(jnp.int32, (layers, columns), 0)
    lane = lax.broadcasted_iota(jnp.int32, (layers, columns), 1)

    def flow_row(src, dst, row, below, above):
        k = half_k[row]
        h = src[row]
        flow = (k + half_k[above]) * (src[above] - h) + (k + half_k[below]) * (src[below] - h)
        side = (k + turn(k, -1, 1)) * (turn(h, -1, 1) - h)
        side = jnp.where(lane == columns - 1, 0.0, side)
        flow = flow + side - turn(side, 1, 1)
        down = (k + turn(k, -1, 0)) * (turn(h, -1, 0) - h - 1.0)
        down = jnp.where(layer == layers - 1, 0.0, down)
        flow = flow + down - turn(down, 1, 0)
        flow = flow - jnp.where(layer == layers - 1, 2.0 * k, 0.0)
        dst[row] = h + flow * gain[row]

    def sweep(src, dst, before_edges, after_edges):
        @pl.loop(1, rows + 1)
        def _(row):
            conduct_row(src, row, True)

        before_edges()
        conduct_row(src, 0, False)
        conduct_row(src, last_row, False)
        flow_row(src, dst, 1, low, 2)
        flow_row(src, dst, rows, rows - 1, high)
        after_edges()

        @pl.loop(2, rows)
        def _(row):
            flow_row(src, dst, row, row - 1, row + 1)

    await_recv(SOIL_C, classes.at[0], classes.at[1])
    await_recv(SOIL_K, ks.at[0], ks.at[last_row])
    soil_row(0, classes[0])
    soil_row(last_row, classes[1])
    ks[0] = 0.5 * ks[0]
    ks[last_row] = 0.5 * ks[last_row]
    await_recv(HEAD_A, head_a.at[0], head_a.at[last_row])
    await_send(SOIL_C, class_in.at[0], class_in.at[rows - 1])
    await_send(SOIL_K, ks_in.at[0], ks_in.at[rows - 1])
    await_send(HEAD_A, head_in.at[0], head_in.at[rows - 1])

    own = slice(rows, 2 * rows)
    wide_lane = lax.broadcasted_iota(jnp.int32, (3 * rows, columns), 1)
    piece = lax.broadcasted_iota(jnp.int32, (3 * rows, LANES), 1) // strip

    def assemble():
        for away in range(1, count):
            spread(away).wait()
        for group in range(groups):
            for kind in range(4):
                joined = None
                for part in range(per):
                    block = turn(gathered[group * per + part], (part - kind) * strip, 1)
                    joined = block if joined is None else jnp.where(piece == part, block, joined)
                spot = slice(group * LANES, (group + 1) * LANES)
                if kind < 3:
                    maps[kind, :, spot] = joined
                else:
                    levels[0, :, spot] = joined

    def shifted(values, first, second):
        values = turn(values, -second, 1)
        if second == 1:
            values = jnp.where(wide_lane == columns - 1, 0.0, values)
        if second == -1:
            values = jnp.where(wide_lane == 0, 0.0, values)
        return turn(values, -first, 0)

    def surface(level, depth):
        coef, erode, code = maps[0], maps[1], maps[2]
        target = jnp.zeros_like(level)
        scale = jnp.ones_like(level)
        for course in range(8):
            first, second = SHIFT_X[course], SHIFT_Y[course]
            chosen = code == course
            target = jnp.where(chosen, shifted(level, first, second), target)
            if first * second != 0:
                scale = jnp.where(chosen, 1.0 / math.sqrt(2.0), scale)
        slope = MIN_SLOPE + jnp.maximum(level - target, 0.0) * scale
        root = jnp.sqrt(slope)
        power = lax.exp2((2.0 / 3.0) * lax.log2(jnp.maximum(depth, TINY)))
        drive = coef * root * power
        outflow = depth * drive / (1.0 + drive)
        sediment = erode * outflow * root
        sums = []
        for field in (outflow, sediment):
            total = -field
            for course in range(8):
                sent = jnp.where(code == course, field, 0.0)
                total = total + shifted(sent, -SHIFT_X[course], -SHIFT_Y[course])
            sums.append(total)
        return sums[0], BED_RATE * sums[1]

    @pl.loop(0, STEPS)
    def _(step):
        slot = lax.rem(step, 2)
        other = 1 - slot
        going = step < STEPS - 1

        def push_b():
            push(HEAD_B, head_b.at[1], head_b.at[rows], head_b.at[0], head_b.at[last_row])

        def take_b():
            await_recv(HEAD_B, head_b.at[0], head_b.at[last_row])
            await_send(HEAD_B, head_b.at[1], head_b.at[rows])

        def push_a():
            @pl.when(going)
            def _():
                push(HEAD_A, head_a.at[1], head_a.at[rows], head_a.at[0], head_a.at[last_row])

        sweep(head_a, head_b, lambda: None, push_b)
        sweep(head_b, head_a, take_b, push_a)

        @pl.when(step == 0)
        def _():
            assemble()

        low_level = levels.at[slot, 0:rows]
        own_level = levels.at[slot, own]
        high_level = levels.at[slot, 2 * rows : 3 * rows]

        @pl.when(step > 0)
        def _():
            await_recv(LEVEL, low_level, high_level)
            await_send(LEVEL, own_level, own_level)

        for row in range(rows):
            depths[rows + row : rows + row + 1] = jnp.maximum(head_a[row + 1, 0:1, :], 0.0)
        low_depth = depths.at[0:rows]
        own_depth = depths.at[own]
        high_depth = depths.at[2 * rows : 3 * rows]
        push(DEPTH, own_depth, own_depth, low_depth, high_depth)
        await_recv(DEPTH, low_depth, high_depth)
        await_send(DEPTH, own_depth, own_depth)

        @pl.when(going)
        def _():
            await_recv(HEAD_A, head_a.at[0], head_a.at[last_row])
            await_send(HEAD_A, head_a.at[1], head_a.at[rows])

        change, bed_change = surface(levels[slot], depths[...])
        for row in range(rows + 2):
            top = head_a[row, 0:1, :]
            head_a[row, 0:1, :] = top + change[rows - 1 + row : rows + row]
        levels[other, own] = levels[slot, own] + bed_change[own]

        @pl.when(going)
        def _():
            next_level = levels.at[other, own]
            push(
                LEVEL,
                next_level,
                next_level,
                levels.at[other, 0:rows],
                levels.at[other, 2 * rows : 3 * rows],
            )

    for group in range(groups):
        final_src[group] = levels[STEPS % 2, own, group * LANES : (group + 1) * LANES]

    def finish(away):
        peer = lax.rem(me + away, count)
        return pltpu.make_async_remote_copy(
            src_ref=final_src.at[peer // per],
            dst_ref=final_dst.at[me],
            send_sem=final_send.at[away],
            recv_sem=final_recv.at[away],
            device_id=at(peer),
            device_id_type=pl.DeviceIdType.MESH,
        )

    for away in range(1, count):
        finish(away).start()
    final_dst[me] = final_src[me // per]
    head_out[...] = head_a[1 : rows + 1]
    for away in range(1, count):
        finish(away).wait()
    members = LANES // rows
    for block in range(width // LANES):
        part = final_dst[block * members : (block + 1) * members]
        turned[:, block * LANES : (block + 1) * LANES] = jnp.transpose(
            part.reshape(LANES, LANES)
        )
    start = pl.multiple_of(lax.rem(me, per) * strip, strip)
    bed_out[...] = turned[pl.ds(start, strip)]


def on_device(
    pressure,
    conductivity,
    soil_class,
    vg_alpha,
    vg_shape,
    bed,
    flow_code,
    surface_soil,
    cover_class,
    ponding,
    conveyance,
    erodibility,
):
    count = lax.axis_size("tile")
    layers, rows, columns = pressure.shape
    strip, width = bed.shape
    head = jnp.swapaxes(pressure, 0, 1)
    ks = jnp.swapaxes(conductivity, 0, 1)
    classes = jnp.swapaxes(soil_class, 0, 1).astype(jnp.float32)
    vmem = pl.BlockSpec(memory_space=pltpu.VMEM)
    smem = pl.BlockSpec(memory_space=pltpu.SMEM)
    wide = pltpu.VMEM((rows + 2, layers, columns), jnp.float32)
    dma = pltpu.SemaphoreType.DMA
    head_out, bed_out = pl.pallas_call(
        functools.partial(kernel, count),
        out_shape=(
            jax.ShapeDtypeStruct((rows, layers, columns), jnp.float32),
            jax.ShapeDtypeStruct((strip, width), jnp.float32),
        ),
        in_specs=[vmem, vmem, vmem, smem, smem, vmem, vmem, vmem, vmem, vmem, smem, smem],
        out_specs=(vmem, vmem),
        scratch_shapes=[
            wide,
            wide,
            wide,
            wide,
            wide,
            wide,
            wide,
            wide,
            pltpu.VMEM((2, 3 * rows, columns), jnp.float32),
            pltpu.VMEM((3 * rows, columns), jnp.float32),
            pltpu.VMEM((3, 3 * rows, columns), jnp.float32),
            pltpu.VMEM((2, layers, columns), jnp.float32),
            pltpu.VMEM((width + 2 * rows, LANES), jnp.float32),
            pltpu.VMEM((count, 3 * rows, LANES), jnp.float32),
            pltpu.VMEM((columns // LANES, rows, LANES), jnp.float32),
            pltpu.VMEM((count, rows, LANES), jnp.float32),
            pltpu.VMEM((LANES, width), jnp.float32),
            dma((6, 2)),
            dma((6, 2)),
            dma((count,)),
            dma((count,)),
            dma((count,)),
            dma((count,)),
        ],
        compiler_params=pltpu.CompilerParams(
            collective_id=0, has_side_effects=True, vmem_limit_bytes=40 * 1024 * 1024
        ),
    )(
        head,
        ks,
        classes,
        vg_alpha,
        vg_shape,
        bed,
        flow_code,
        surface_soil,
        cover_class,
        ponding,
        conveyance,
        erodibility,
    )
    return jnp.swapaxes(head_out, 0, 1), bed_out


def solution(mesh):
    in_specs = (
        P("member", "tile", None),
        P("member", "tile", None),
        P("member", "tile", None),
        P(),
        P(),
        P("tile", "member"),
        P("tile", "member"),
        P("tile", "member"),
        P("tile", "member"),
        P("tile", "member"),
        P(),
        P(),
    )
    out_specs = (P("member", "tile", None), P("tile", "member"))
    return jax.shard_map(
        on_device, mesh=mesh, in_specs=in_specs, out_specs=out_specs, check_vma=False
    )
```

```python
import functools
import math

import jax
import jax.numpy as jnp
from jax import lax
from jax.experimental import pallas as pl
from jax.experimental.pallas import tpu as pltpu
from jax.sharding import PartitionSpec as P

STEPS = 4
RELAX_STEP = 0.08
CAPACITY = 2.0
MIN_SLOPE = 0.01
BED_RATE = 2.0
SHIFT_X = (1, 1, 0, -1, -1, -1, 0, 1)
SHIFT_Y = (0, 1, 1, 1, 0, -1, -1, -1)
TINY = 1.2e-38
LANES = 128
TOPS, REST, LEVEL, SOIL_K, SOIL_C = range(5)
HALO = 2
TOP = 8


def table_pick(classes, table, entries):
    picked = jnp.full(classes.shape, table(0), jnp.float32)
    for entry in range(1, entries):
        picked = jnp.where(classes == entry, table(entry), picked)
    return picked


def turn(values, shift, axis):
    shift = shift % values.shape[axis]
    return values if shift == 0 else pltpu.roll(values, shift, axis)


def kernel(
    count,
    head_in,
    ks_in,
    class_in,
    alpha_t,
    shape_t,
    bed_in,
    code_in,
    soil_in,
    cover_in,
    pond_in,
    convey_t,
    erod_t,
    head_out,
    bed_out,
    head_a,
    head_b,
    half_k,
    gain,
    ks,
    alpha,
    shape,
    half_m,
    levels,
    depths,
    maps,
    classes,
    tops,
    rest,
    packed,
    gathered,
    final_src,
    final_dst,
    turned,
    send_sem,
    recv_sem,
    spread_send,
    spread_recv,
    final_send,
    final_recv,
):
    rows, layers, columns = head_in.shape
    strip = bed_in.shape[0]
    width = bed_in.shape[1]
    per = LANES // strip
    groups = columns // LANES
    me = lax.axis_index("tile")
    has_left = me > 0
    has_right = me < count - 1
    first = HALO
    last = rows + HALO - 1
    total_rows = rows + 2 * HALO
    low = first - (me + count - 1) // count
    high = last + (2 * count - 2 - me) // count

    def at(tile):
        return {"tile": tile}

    def to_left(kind, slot, src, dst):
        return pltpu.make_async_remote_copy(
            src_ref=src,
            dst_ref=dst,
            send_sem=send_sem.at[kind, slot, 0],
            recv_sem=recv_sem.at[kind, slot, 1],
            device_id=at(me - 1),
            device_id_type=pl.DeviceIdType.MESH,
        )

    def to_right(kind, slot, src, dst):
        return pltpu.make_async_remote_copy(
            src_ref=src,
            dst_ref=dst,
            send_sem=send_sem.at[kind, slot, 1],
            recv_sem=recv_sem.at[kind, slot, 0],
            device_id=at(me + 1),
            device_id_type=pl.DeviceIdType.MESH,
        )

    def push(kind, slot, for_left, for_right, low_halo, high_halo):
        @pl.when(has_left)
        def _():
            to_left(kind, slot, for_left, high_halo).start()

        @pl.when(has_right)
        def _():
            to_right(kind, slot, for_right, low_halo).start()

    def settle(kind, slot, low_halo, high_halo):
        @pl.when(has_left)
        def _():
            to_right(kind, slot, low_halo, low_halo).wait_recv()
            to_left(kind, slot, low_halo, low_halo).wait_send()

        @pl.when(has_right)
        def _():
            to_left(kind, slot, high_halo, high_halo).wait_recv()
            to_right(kind, slot, high_halo, high_halo).wait_send()

    levels[...] = jnp.zeros_like(levels)
    depths[...] = jnp.zeros_like(depths)
    tops[...] = jnp.zeros_like(tops)

    barrier = pltpu.get_barrier_semaphore()
    for away in range(1, count):
        pl.semaphore_signal(
            barrier,
            inc=1,
            device_id=at(lax.rem(me + away, count)),
            device_id_type=pl.DeviceIdType.MESH,
        )
    coef_y = table_pick(cover_in[...], lambda i: convey_t[i], convey_t.shape[0]) * (
        1.0 - pond_in[...].astype(jnp.float32)
    )
    erode_y = table_pick(soil_in[...], lambda i: erod_t[i], erod_t.shape[0])
    stacked = jnp.concatenate(
        [coef_y, erode_y, code_in[...].astype(jnp.float32), bed_in[...]], axis=0
    )
    packed[0:rows] = jnp.zeros((rows, LANES), jnp.float32)
    packed[rows + width : 2 * rows + width] = jnp.zeros((rows, LANES), jnp.float32)
    for block in range(width // LANES):
        packed[rows + block * LANES : rows + (block + 1) * LANES] = jnp.transpose(
            stacked[:, block * LANES : (block + 1) * LANES]
        )

    def soil_row(row, found):
        alpha[row] = table_pick(found, lambda i: alpha_t[i], alpha_t.shape[0])
        bend = table_pick(found, lambda i: shape_t[i], shape_t.shape[0])
        shape[row] = bend
        half_m[row] = 0.5 / bend - 0.5

    def conduct_row(head, row, part):
        bend = shape[row, part]
        log_a = lax.log2(alpha[row, part] * jnp.maximum(-head[row, part], TINY))
        log_w = lax.log2(1.0 + lax.exp2(bend * log_a))
        root = lax.exp2(half_m[row, part] * log_w)
        full = root * root
        inner = 1.0 - lax.exp2((bend - 1.0) * log_a) * full
        half_k[row, part] = ks[row, part] * root * (inner * inner)
        gain[row, part] = RELAX_STEP / (1.0 + CAPACITY * (1.0 - full))

    layer = lax.broadcasted_iota(jnp.int32, (layers, columns), 0)
    lane = lax.broadcasted_iota(jnp.int32, (layers, columns), 1)

    def flow_row(src, dst, row, below, above):
        k = half_k[row]
        h = src[row]
        flow = (k + half_k[above]) * (src[above] - h) + (k + half_k[below]) * (src[below] - h)
        side = (k + turn(k, -1, 1)) * (turn(h, -1, 1) - h)
        side = jnp.where(lane == columns - 1, 0.0, side)
        flow = flow + side - turn(side, 1, 1)
        down = (k + turn(k, -1, 0)) * (turn(h, -1, 0) - h - 1.0)
        down = jnp.where(layer == layers - 1, 0.0, down)
        flow = flow + down - turn(down, 1, 0)
        flow = flow - jnp.where(layer == layers - 1, 2.0 * k, 0.0)
        dst[row] = h + flow * gain[row]

    whole_part = slice(0, layers)
    top_part = slice(0, TOP)
    rest_part = slice(TOP, layers)

    def conduct_rows(head, start, stop, part):
        @pl.loop(start, stop, unroll=True)
        def _(row):
            conduct_row(head, row, part)

    @pl.loop(0, rows)
    def _(row):
        soil_row(row + first, class_in[row])
        ks[row + first] = 0.5 * ks_in[row]
        head_a[row + first] = head_in[row]

    pl.semaphore_wait(barrier, count - 1)

    early, late = slice(0, HALO), slice(rows - HALO, rows)
    above_own = slice(last + 1, total_rows)
    push(
        REST,
        0,
        head_in.at[early, rest_part],
        head_in.at[late, rest_part],
        rest.at[0, 0],
        rest.at[0, 1],
    )
    push(
        TOPS,
        0,
        head_in.at[0 : HALO + 1, top_part],
        head_in.at[rows - HALO - 1 : rows, top_part],
        tops.at[0, 0],
        tops.at[0, 1],
    )
    push(SOIL_C, 0, class_in.at[early], class_in.at[late], classes.at[0], classes.at[1])
    push(SOIL_K, 0, ks_in.at[early], ks_in.at[late], ks.at[0:HALO], ks.at[above_own])

    def spread(away):
        peer = lax.rem(me + away, count)
        return pltpu.make_async_remote_copy(
            src_ref=packed.at[pl.ds(pl.multiple_of(peer * rows, rows), 3 * rows)],
            dst_ref=gathered.at[me],
            send_sem=spread_send.at[away],
            recv_sem=spread_recv.at[away],
            device_id=at(peer),
            device_id_type=pl.DeviceIdType.MESH,
        )

    for away in range(1, count):
        spread(away).start()
    gathered[me] = packed[pl.ds(pl.multiple_of(me * rows, rows), 3 * rows)]

    own = slice(rows, 2 * rows)
    wide_lane = lax.broadcasted_iota(jnp.int32, (3 * rows, columns), 1)
    piece = lax.broadcasted_iota(jnp.int32, (3 * rows, LANES), 1) // strip

    def assemble():
        for away in range(1, count):
            spread(away).wait()
        for group in range(groups):
            for kind in range(4):
                joined = None
                for part in range(per):
                    block = turn(gathered[group * per + part], (part - kind) * strip, 1)
                    joined = block if joined is None else jnp.where(piece == part, block, joined)
                spot = slice(group * LANES, (group + 1) * LANES)
                if kind < 3:
                    maps[kind, :, spot] = joined
                else:
                    levels[0, :, spot] = joined

    def shifted(values, first, second):
        values = turn(values, -second, 1)
        if second == 1:
            values = jnp.where(wide_lane == columns - 1, 0.0, values)
        if second == -1:
            values = jnp.where(wide_lane == 0, 0.0, values)
        return turn(values, -first, 0)

    def surface(level, depth):
        coef, erode, code = maps[0], maps[1], maps[2]
        target = jnp.zeros_like(level)
        scale = jnp.ones_like(level)
        for course in range(8):
            first, second = SHIFT_X[course], SHIFT_Y[course]
            chosen = code == course
            target = jnp.where(chosen, shifted(level, first, second), target)
            if first * second != 0:
                scale = jnp.where(chosen, 1.0 / math.sqrt(2.0), scale)
        slope = MIN_SLOPE + jnp.maximum(level - target, 0.0) * scale
        root = jnp.sqrt(slope)
        power = lax.exp2((2.0 / 3.0) * lax.log2(jnp.maximum(depth, TINY)))
        drive = coef * root * power
        outflow = depth * drive / (1.0 + drive)
        sediment = erode * outflow * root
        sums = []
        for field in (outflow, sediment):
            total = -field
            for course in range(8):
                sent = jnp.where(code == course, field, 0.0)
                total = total + shifted(sent, -SHIFT_X[course], -SHIFT_Y[course])
            sums.append(total)
        return sums[0], BED_RATE * sums[1]

    def surface_halo(slot):
        for side in range(HALO):
            head_a[side, top_part] = tops[slot, 0, side + 1]
            head_a[last + 1 + side, top_part] = tops[slot, 1, side]

    conduct_rows(head_a, first, last + 1, rest_part)

    @pl.loop(0, STEPS)
    def _(step):
        slot = lax.rem(step, 2)
        other = 1 - slot
        going = step < STEPS - 1

        conduct_rows(head_a, first, last + 1, top_part)
        for row in range(first + 1, last):
            flow_row(head_a, head_b, row, row - 1, row + 1)

        @pl.when(step == 0)
        def _():
            settle(TOPS, 0, tops.at[0, 0], tops.at[0, 1])
            surface_halo(0)
            settle(SOIL_C, 0, classes.at[0], classes.at[1])
            settle(SOIL_K, 0, ks.at[0:HALO], ks.at[above_own])
            for side in range(HALO):
                for row, found in ((side, classes[0, side]), (last + 1 + side, classes[1, side])):
                    soil_row(row, found)
                    ks[row] = 0.5 * ks[row]

        settle(REST, slot, rest.at[slot, 0], rest.at[slot, 1])
        for side in range(HALO):
            head_a[side, rest_part] = rest[slot, 0, side]
            head_a[last + 1 + side, rest_part] = rest[slot, 1, side]
        conduct_rows(head_a, 0, HALO, whole_part)
        conduct_rows(head_a, last + 1, total_rows, whole_part)
        flow_row(head_a, head_b, first, low, first + 1)
        flow_row(head_a, head_b, last, last - 1, high)
        flow_row(head_a, head_b, first - 1, first - 2, first)
        flow_row(head_a, head_b, last + 1, last, last + 2)

        conduct_rows(head_b, first - 1, last + 2, whole_part)
        for row in range(first, last + 1):
            if row <= first + HALO or row >= last - HALO:
                below = low if row == first else row - 1
                above = high if row == last else row + 1
                flow_row(head_b, head_a, row, below, above)
        push(
            TOPS,
            other,
            head_a.at[first : first + HALO + 1, top_part],
            head_a.at[last - HALO : last + 1, top_part],
            tops.at[other, 0],
            tops.at[other, 1],
        )

        @pl.when(going)
        def _():
            push(
                REST,
                other,
                head_a.at[first : first + HALO, rest_part],
                head_a.at[last - HALO + 1 : last + 1, rest_part],
                rest.at[other, 0],
                rest.at[other, 1],
            )

        for row in range(first + HALO + 1, last - HALO):
            flow_row(head_b, head_a, row, row - 1, row + 1)

        @pl.when(going)
        def _():
            conduct_rows(head_a, first, last + 1, rest_part)

        @pl.when(step == 0)
        def _():
            assemble()

        @pl.when(step > 0)
        def _():
            settle(
                LEVEL, slot, levels.at[slot, 0:rows], levels.at[slot, 2 * rows : 3 * rows]
            )

        for row in range(rows):
            depths[rows + row : rows + row + 1] = jnp.maximum(head_a[row + first, 0:1, :], 0.0)
        settle(TOPS, other, tops.at[other, 0], tops.at[other, 1])
        for side in range(HALO + 1):
            spot = rows - HALO - 1 + side
            depths[spot : spot + 1] = jnp.maximum(tops[other, 0, side, 0:1, :], 0.0)
            spot = 2 * rows + side
            depths[spot : spot + 1] = jnp.maximum(tops[other, 1, side, 0:1, :], 0.0)

        change, bed_change = surface(levels[slot], depths[...])
        surface_halo(other)
        for row in range(total_rows):
            spot = rows - first + row
            head_a[row, 0:1, :] = head_a[row, 0:1, :] + change[spot : spot + 1]
        levels[other, own] = levels[slot, own] + bed_change[own]

        @pl.when(going)
        def _():
            next_level = levels.at[other, own]
            push(
                LEVEL,
                other,
                next_level,
                next_level,
                levels.at[other, 0:rows],
                levels.at[other, 2 * rows : 3 * rows],
            )

    for group in range(groups):
        final_src[group] = levels[STEPS % 2, own, group * LANES : (group + 1) * LANES]

    def finish(away):
        peer = lax.rem(me + away, count)
        return pltpu.make_async_remote_copy(
            src_ref=final_src.at[peer // per],
            dst_ref=final_dst.at[me],
            send_sem=final_send.at[away],
            recv_sem=final_recv.at[away],
            device_id=at(peer),
            device_id_type=pl.DeviceIdType.MESH,
        )

    for away in range(1, count):
        finish(away).start()
    final_dst[me] = final_src[me // per]
    head_out[...] = head_a[first : last + 1]
    for away in range(1, count):
        finish(away).wait()
    members = LANES // rows
    for block in range(width // LANES):
        part = final_dst[block * members : (block + 1) * members]
        turned[:, block * LANES : (block + 1) * LANES] = jnp.transpose(
            part.reshape(LANES, LANES)
        )
    start = pl.multiple_of(lax.rem(me, per) * strip, strip)
    bed_out[...] = turned[pl.ds(start, strip)]


def on_device(
    pressure,
    conductivity,
    soil_class,
    vg_alpha,
    vg_shape,
    bed,
    flow_code,
    surface_soil,
    cover_class,
    ponding,
    conveyance,
    erodibility,
):
    count = lax.axis_size("tile")
    layers, rows, columns = pressure.shape
    strip, width = bed.shape
    head = jnp.swapaxes(pressure, 0, 1)
    ks = jnp.swapaxes(conductivity, 0, 1)
    classes = jnp.swapaxes(soil_class, 0, 1).astype(jnp.float32)
    vmem = pl.BlockSpec(memory_space=pltpu.VMEM)
    smem = pl.BlockSpec(memory_space=pltpu.SMEM)
    wide = pltpu.VMEM((rows + 2 * HALO, layers, columns), jnp.float32)
    dma = pltpu.SemaphoreType.DMA
    head_out, bed_out = pl.pallas_call(
        functools.partial(kernel, count),
        out_shape=(
            jax.ShapeDtypeStruct((rows, layers, columns), jnp.float32),
            jax.ShapeDtypeStruct((strip, width), jnp.float32),
        ),
        in_specs=[vmem, vmem, vmem, smem, smem, vmem, vmem, vmem, vmem, vmem, smem, smem],
        out_specs=(vmem, vmem),
        scratch_shapes=[
            wide,
            wide,
            wide,
            wide,
            wide,
            wide,
            wide,
            wide,
            pltpu.VMEM((2, 3 * rows, columns), jnp.float32),
            pltpu.VMEM((3 * rows, columns), jnp.float32),
            pltpu.VMEM((3, 3 * rows, columns), jnp.float32),
            pltpu.VMEM((2, HALO, layers, columns), jnp.float32),
            pltpu.VMEM((2, 2, HALO + 1, TOP, columns), jnp.float32),
            pltpu.VMEM((2, 2, HALO, layers - TOP, columns), jnp.float32),
            pltpu.VMEM((width + 2 * rows, LANES), jnp.float32),
            pltpu.VMEM((count, 3 * rows, LANES), jnp.float32),
            pltpu.VMEM((columns // LANES, rows, LANES), jnp.float32),
            pltpu.VMEM((count, rows, LANES), jnp.float32),
            pltpu.VMEM((LANES, width), jnp.float32),
            dma((5, 2, 2)),
            dma((5, 2, 2)),
            dma((count,)),
            dma((count,)),
            dma((count,)),
            dma((count,)),
        ],
        compiler_params=pltpu.CompilerParams(
            collective_id=0, has_side_effects=True, vmem_limit_bytes=40 * 1024 * 1024
        ),
    )(
        head,
        ks,
        classes,
        vg_alpha,
        vg_shape,
        bed,
        flow_code,
        surface_soil,
        cover_class,
        ponding,
        conveyance,
        erodibility,
    )
    return jnp.swapaxes(head_out, 0, 1), bed_out


def solution(mesh):
    in_specs = (
        P("member", "tile", None),
        P("member", "tile", None),
        P("member", "tile", None),
        P(),
        P(),
        P("tile", "member"),
        P("tile", "member"),
        P("tile", "member"),
        P("tile", "member"),
        P("tile", "member"),
        P(),
        P(),
    )
    out_specs = (P("member", "tile", None), P("tile", "member"))
    return jax.shard_map(
        on_device, mesh=mesh, in_specs=in_specs, out_specs=out_specs, check_vma=False
    )
```

```python
import functools
import math

import jax
import jax.numpy as jnp
from jax import lax
from jax.experimental import pallas as pl
from jax.experimental.pallas import tpu as pltpu
from jax.sharding import PartitionSpec as P

STEPS = 4
RELAX_STEP = 0.08
CAPACITY = 2.0
MIN_SLOPE = 0.01
BED_RATE = 2.0
SHIFT_X = (1, 1, 0, -1, -1, -1, 0, 1)
SHIFT_Y = (0, 1, 1, 1, 0, -1, -1, -1)
TINY = 1.2e-38
LANES = 128
TOPS, REST, LEVEL, SOIL_K, SOIL_C, DEPTH = range(6)
HALO = 2
TOP = 8


def table_pick(classes, table, entries):
    picked = jnp.full(classes.shape, table(0), jnp.float32)
    for entry in range(1, entries):
        picked = jnp.where(classes == entry, table(entry), picked)
    return picked


def turn(values, shift, axis):
    shift = shift % values.shape[axis]
    return values if shift == 0 else pltpu.roll(values, shift, axis)


def kernel(
    count,
    head_in,
    ks_in,
    class_in,
    alpha_t,
    shape_t,
    bed_in,
    code_in,
    soil_in,
    cover_in,
    pond_in,
    convey_t,
    erod_t,
    head_out,
    bed_out,
    head_a,
    head_b,
    half_k,
    gain,
    ks,
    alpha,
    shape,
    half_m,
    levels,
    depths,
    maps,
    classes,
    tops,
    rest,
    edge,
    edges,
    halo_change,
    packed,
    gathered,
    final_src,
    final_dst,
    turned,
    send_sem,
    recv_sem,
    spread_send,
    spread_recv,
    final_send,
    final_recv,
):
    rows, layers, columns = head_in.shape
    strip = bed_in.shape[0]
    width = bed_in.shape[1]
    per = LANES // strip
    groups = columns // LANES
    me = lax.axis_index("tile")
    has_left = me > 0
    has_right = me < count - 1
    first = HALO
    last = rows + HALO - 1
    total_rows = rows + 2 * HALO
    low = first - (me + count - 1) // count
    high = last + (2 * count - 2 - me) // count

    def at(tile):
        return {"tile": tile}

    def to_left(kind, slot, src, dst):
        return pltpu.make_async_remote_copy(
            src_ref=src,
            dst_ref=dst,
            send_sem=send_sem.at[kind, slot, 0],
            recv_sem=recv_sem.at[kind, slot, 1],
            device_id=at(me - 1),
            device_id_type=pl.DeviceIdType.MESH,
        )

    def to_right(kind, slot, src, dst):
        return pltpu.make_async_remote_copy(
            src_ref=src,
            dst_ref=dst,
            send_sem=send_sem.at[kind, slot, 1],
            recv_sem=recv_sem.at[kind, slot, 0],
            device_id=at(me + 1),
            device_id_type=pl.DeviceIdType.MESH,
        )

    def push(kind, slot, for_left, for_right, low_halo, high_halo):
        @pl.when(has_left)
        def _():
            to_left(kind, slot, for_left, high_halo).start()

        @pl.when(has_right)
        def _():
            to_right(kind, slot, for_right, low_halo).start()

    def settle(kind, slot, low_halo, high_halo, recv=True, send=True):
        @pl.when(has_left)
        def _():
            if recv:
                to_right(kind, slot, low_halo, low_halo).wait_recv()
            if send:
                to_left(kind, slot, low_halo, low_halo).wait_send()

        @pl.when(has_right)
        def _():
            if recv:
                to_left(kind, slot, high_halo, high_halo).wait_recv()
            if send:
                to_right(kind, slot, high_halo, high_halo).wait_send()

    levels[...] = jnp.zeros_like(levels)
    depths[...] = jnp.zeros_like(depths)
    edge[...] = jnp.zeros_like(edge)
    edges[...] = jnp.zeros_like(edges)
    halo_change[...] = jnp.zeros_like(halo_change)

    barrier = pltpu.get_barrier_semaphore()
    for away in range(1, count):
        pl.semaphore_signal(
            barrier,
            inc=1,
            device_id=at(lax.rem(me + away, count)),
            device_id_type=pl.DeviceIdType.MESH,
        )
    coef_y = table_pick(cover_in[...], lambda i: convey_t[i], convey_t.shape[0]) * (
        1.0 - pond_in[...].astype(jnp.float32)
    )
    erode_y = table_pick(soil_in[...], lambda i: erod_t[i], erod_t.shape[0])
    stacked = jnp.concatenate(
        [coef_y, erode_y, code_in[...].astype(jnp.float32), bed_in[...]], axis=0
    )
    packed[0:rows] = jnp.zeros((rows, LANES), jnp.float32)
    packed[rows + width : 2 * rows + width] = jnp.zeros((rows, LANES), jnp.float32)
    for block in range(width // LANES):
        packed[rows + block * LANES : rows + (block + 1) * LANES] = jnp.transpose(
            stacked[:, block * LANES : (block + 1) * LANES]
        )

    def soil_row(row, found):
        alpha[row] = table_pick(found, lambda i: alpha_t[i], alpha_t.shape[0])
        bend = table_pick(found, lambda i: shape_t[i], shape_t.shape[0])
        shape[row] = bend
        half_m[row] = 0.5 / bend - 0.5

    def conduct_row(head, row, part):
        bend = shape[row, part]
        log_a = lax.log2(alpha[row, part] * jnp.maximum(-head[row, part], TINY))
        log_w = lax.log2(1.0 + lax.exp2(bend * log_a))
        root = lax.exp2(half_m[row, part] * log_w)
        full = root * root
        inner = 1.0 - lax.exp2((bend - 1.0) * log_a) * full
        half_k[row, part] = ks[row, part] * root * (inner * inner)
        gain[row, part] = RELAX_STEP / (1.0 + CAPACITY * (1.0 - full))

    layer = lax.broadcasted_iota(jnp.int32, (layers, columns), 0)
    lane = lax.broadcasted_iota(jnp.int32, (layers, columns), 1)

    def flow_row(src, dst, row, below, above):
        k = half_k[row]
        h = src[row]
        flow = (k + half_k[above]) * (src[above] - h) + (k + half_k[below]) * (src[below] - h)
        side = (k + turn(k, -1, 1)) * (turn(h, -1, 1) - h)
        side = jnp.where(lane == columns - 1, 0.0, side)
        flow = flow + side - turn(side, 1, 1)
        down = (k + turn(k, -1, 0)) * (turn(h, -1, 0) - h - 1.0)
        down = jnp.where(layer == layers - 1, 0.0, down)
        flow = flow + down - turn(down, 1, 0)
        flow = flow - jnp.where(layer == layers - 1, 2.0 * k, 0.0)
        dst[row] = h + flow * gain[row]

    whole_part = slice(0, layers)
    top_part = slice(0, TOP)
    rest_part = slice(TOP, layers)

    def conduct_rows(head, start, stop, part):
        @pl.loop(start, stop, unroll=True)
        def _(row):
            conduct_row(head, row, part)

    @pl.loop(0, rows)
    def _(row):
        soil_row(row + first, class_in[row])
        ks[row + first] = 0.5 * ks_in[row]
        head_a[row + first] = head_in[row]

    pl.semaphore_wait(barrier, count - 1)

    early, late = slice(0, HALO), slice(rows - HALO, rows)
    above_own = slice(last + 1, total_rows)
    push(
        REST,
        0,
        head_in.at[early, rest_part],
        head_in.at[late, rest_part],
        rest.at[0, 0],
        rest.at[0, 1],
    )
    push(
        TOPS,
        0,
        head_in.at[early, top_part],
        head_in.at[late, top_part],
        tops.at[0, 0],
        tops.at[0, 1],
    )
    push(SOIL_C, 0, class_in.at[early], class_in.at[late], classes.at[0], classes.at[1])
    push(SOIL_K, 0, ks_in.at[early], ks_in.at[late], ks.at[0:HALO], ks.at[above_own])

    def spread(away):
        peer = lax.rem(me + away, count)
        return pltpu.make_async_remote_copy(
            src_ref=packed.at[pl.ds(pl.multiple_of(peer * rows, rows), 3 * rows)],
            dst_ref=gathered.at[me],
            send_sem=spread_send.at[away],
            recv_sem=spread_recv.at[away],
            device_id=at(peer),
            device_id_type=pl.DeviceIdType.MESH,
        )

    for away in range(1, count):
        spread(away).start()
    gathered[me] = packed[pl.ds(pl.multiple_of(me * rows, rows), 3 * rows)]

    own = slice(rows, 2 * rows)
    wide_lane = lax.broadcasted_iota(jnp.int32, (3 * rows, columns), 1)
    piece = lax.broadcasted_iota(jnp.int32, (3 * rows, LANES), 1) // strip

    def assemble():
        for away in range(1, count):
            spread(away).wait()
        for group in range(groups):
            for kind in range(4):
                joined = None
                for part in range(per):
                    block = turn(gathered[group * per + part], (part - kind) * strip, 1)
                    joined = block if joined is None else jnp.where(piece == part, block, joined)
                spot = slice(group * LANES, (group + 1) * LANES)
                if kind < 3:
                    maps[kind, :, spot] = joined
                else:
                    levels[0, :, spot] = joined

    def shifted(values, first, second):
        values = turn(values, -second, 1)
        if second == 1:
            values = jnp.where(wide_lane == columns - 1, 0.0, values)
        if second == -1:
            values = jnp.where(wide_lane == 0, 0.0, values)
        return turn(values, -first, 0)

    def surface(level, depth):
        coef, erode, code = maps[0], maps[1], maps[2]
        target = jnp.zeros_like(level)
        scale = jnp.ones_like(level)
        for course in range(8):
            first, second = SHIFT_X[course], SHIFT_Y[course]
            chosen = code == course
            target = jnp.where(chosen, shifted(level, first, second), target)
            if first * second != 0:
                scale = jnp.where(chosen, 1.0 / math.sqrt(2.0), scale)
        slope = MIN_SLOPE + jnp.maximum(level - target, 0.0) * scale
        root = jnp.sqrt(slope)
        power = lax.exp2((2.0 / 3.0) * lax.log2(jnp.maximum(depth, TINY)))
        drive = coef * root * power
        outflow = depth * drive / (1.0 + drive)
        sediment = erode * outflow * root
        sums = []
        for field in (outflow, sediment):
            total = -field
            for course in range(8):
                sent = jnp.where(code == course, field, 0.0)
                total = total + shifted(sent, -SHIFT_X[course], -SHIFT_Y[course])
            sums.append(total)
        return sums[0], BED_RATE * sums[1]

    def surface_halo(slot):
        for side in range(HALO):
            head_a[side, top_part] = tops[slot, 0, side]
            head_a[last + 1 + side, top_part] = tops[slot, 1, side]

    conduct_rows(head_a, first, last + 1, rest_part)

    @pl.loop(0, STEPS)
    def _(step):
        slot = lax.rem(step, 2)
        other = 1 - slot
        going = step < STEPS - 1

        conduct_rows(head_a, first, last + 1, top_part)
        for row in range(first + 1, last):
            flow_row(head_a, head_b, row, row - 1, row + 1)

        @pl.when(step == 0)
        def _():
            settle(TOPS, 0, tops.at[0, 0], tops.at[0, 1], recv=False)
            settle(SOIL_C, 0, classes.at[0], classes.at[1])
            settle(SOIL_K, 0, ks.at[0:HALO], ks.at[above_own])
            for side in range(HALO):
                for row, found in ((side, classes[0, side]), (last + 1 + side, classes[1, side])):
                    soil_row(row, found)
                    ks[row] = 0.5 * ks[row]

        settle(TOPS, slot, tops.at[slot, 0], tops.at[slot, 1], send=False)
        surface_halo(slot)
        for side in range(HALO):
            for row, spot in ((side, side), (last + 1 + side, HALO + side)):
                head_a[row, 0:1, :] = head_a[row, 0:1, :] + halo_change[spot : spot + 1]
        settle(REST, slot, rest.at[slot, 0], rest.at[slot, 1])
        for side in range(HALO):
            head_a[side, rest_part] = rest[slot, 0, side]
            head_a[last + 1 + side, rest_part] = rest[slot, 1, side]
        conduct_rows(head_a, 0, HALO, whole_part)
        conduct_rows(head_a, last + 1, total_rows, whole_part)
        flow_row(head_a, head_b, first, low, first + 1)
        flow_row(head_a, head_b, last, last - 1, high)
        flow_row(head_a, head_b, first - 1, first - 2, first)
        flow_row(head_a, head_b, last + 1, last, last + 2)

        conduct_rows(head_b, first - 1, last + 2, whole_part)
        for row in range(first, last + 1):
            if row <= first + HALO or row >= last - HALO:
                below = low if row == first else row - 1
                above = high if row == last else row + 1
                flow_row(head_b, head_a, row, below, above)
        for side in range(HALO + 1):
            edge[side : side + 1] = jnp.maximum(head_a[first + side, 0:1, :], 0.0)
            spot = HALO + 1 + side
            edge[spot : spot + 1] = jnp.maximum(head_a[last - HALO + side, 0:1, :], 0.0)
        push(DEPTH, other, edge, edge, edges.at[other, 0], edges.at[other, 1])

        @pl.when(going)
        def _():
            push(
                TOPS,
                other,
                head_a.at[first : first + HALO, top_part],
                head_a.at[last - HALO + 1 : last + 1, top_part],
                tops.at[other, 0],
                tops.at[other, 1],
            )
            push(
                REST,
                other,
                head_a.at[first : first + HALO, rest_part],
                head_a.at[last - HALO + 1 : last + 1, rest_part],
                rest.at[other, 0],
                rest.at[other, 1],
            )

        for row in range(first + HALO + 1, last - HALO):
            flow_row(head_b, head_a, row, row - 1, row + 1)

        @pl.when(going)
        def _():
            conduct_rows(head_a, first, last + 1, rest_part)

        @pl.when(step == 0)
        def _():
            assemble()

        @pl.when(step > 0)
        def _():
            settle(
                LEVEL, slot, levels.at[slot, 0:rows], levels.at[slot, 2 * rows : 3 * rows]
            )

        for row in range(rows):
            depths[rows + row : rows + row + 1] = jnp.maximum(head_a[row + first, 0:1, :], 0.0)
        settle(DEPTH, other, edges.at[other, 0], edges.at[other, 1])
        span = HALO + 1
        depths[rows - span : rows] = edges[other, 0, span : 2 * span]
        depths[2 * rows : 2 * rows + span] = edges[other, 1, 0:span]

        change, bed_change = surface(levels[slot], depths[...])

        @pl.when(going)
        def _():
            settle(TOPS, other, tops.at[other, 0], tops.at[other, 1], recv=False)

        for row in range(first, last + 1):
            spot = rows - first + row
            head_a[row, 0:1, :] = head_a[row, 0:1, :] + change[spot : spot + 1]
        halo_change[0:HALO] = change[rows - HALO : rows]
        halo_change[HALO : 2 * HALO] = change[2 * rows : 2 * rows + HALO]
        levels[other, own] = levels[slot, own] + bed_change[own]

        @pl.when(going)
        def _():
            next_level = levels.at[other, own]
            push(
                LEVEL,
                other,
                next_level,
                next_level,
                levels.at[other, 0:rows],
                levels.at[other, 2 * rows : 3 * rows],
            )

    for group in range(groups):
        final_src[group] = levels[STEPS % 2, own, group * LANES : (group + 1) * LANES]

    def finish(away):
        peer = lax.rem(me + away, count)
        return pltpu.make_async_remote_copy(
            src_ref=final_src.at[peer // per],
            dst_ref=final_dst.at[me],
            send_sem=final_send.at[away],
            recv_sem=final_recv.at[away],
            device_id=at(peer),
            device_id_type=pl.DeviceIdType.MESH,
        )

    for away in range(1, count):
        finish(away).start()
    final_dst[me] = final_src[me // per]
    head_out[...] = head_a[first : last + 1]
    for away in range(1, count):
        finish(away).wait()
    members = LANES // rows
    for block in range(width // LANES):
        part = final_dst[block * members : (block + 1) * members]
        turned[:, block * LANES : (block + 1) * LANES] = jnp.transpose(
            part.reshape(LANES, LANES)
        )
    start = pl.multiple_of(lax.rem(me, per) * strip, strip)
    bed_out[...] = turned[pl.ds(start, strip)]


def on_device(
    pressure,
    conductivity,
    soil_class,
    vg_alpha,
    vg_shape,
    bed,
    flow_code,
    surface_soil,
    cover_class,
    ponding,
    conveyance,
    erodibility,
):
    count = lax.axis_size("tile")
    layers, rows, columns = pressure.shape
    strip, width = bed.shape
    head = jnp.swapaxes(pressure, 0, 1)
    ks = jnp.swapaxes(conductivity, 0, 1)
    classes = jnp.swapaxes(soil_class, 0, 1).astype(jnp.float32)
    vmem = pl.BlockSpec(memory_space=pltpu.VMEM)
    smem = pl.BlockSpec(memory_space=pltpu.SMEM)
    wide = pltpu.VMEM((rows + 2 * HALO, layers, columns), jnp.float32)
    dma = pltpu.SemaphoreType.DMA
    head_out, bed_out = pl.pallas_call(
        functools.partial(kernel, count),
        out_shape=(
            jax.ShapeDtypeStruct((rows, layers, columns), jnp.float32),
            jax.ShapeDtypeStruct((strip, width), jnp.float32),
        ),
        in_specs=[vmem, vmem, vmem, smem, smem, vmem, vmem, vmem, vmem, vmem, smem, smem],
        out_specs=(vmem, vmem),
        scratch_shapes=[
            wide,
            wide,
            wide,
            wide,
            wide,
            wide,
            wide,
            wide,
            pltpu.VMEM((2, 3 * rows, columns), jnp.float32),
            pltpu.VMEM((3 * rows, columns), jnp.float32),
            pltpu.VMEM((3, 3 * rows, columns), jnp.float32),
            pltpu.VMEM((2, HALO, layers, columns), jnp.float32),
            pltpu.VMEM((2, 2, HALO, TOP, columns), jnp.float32),
            pltpu.VMEM((2, 2, HALO, layers - TOP, columns), jnp.float32),
            pltpu.VMEM((TOP, columns), jnp.float32),
            pltpu.VMEM((2, 2, TOP, columns), jnp.float32),
            pltpu.VMEM((TOP, columns), jnp.float32),
            pltpu.VMEM((width + 2 * rows, LANES), jnp.float32),
            pltpu.VMEM((count, 3 * rows, LANES), jnp.float32),
            pltpu.VMEM((columns // LANES, rows, LANES), jnp.float32),
            pltpu.VMEM((count, rows, LANES), jnp.float32),
            pltpu.VMEM((LANES, width), jnp.float32),
            dma((6, 2, 2)),
            dma((6, 2, 2)),
            dma((count,)),
            dma((count,)),
            dma((count,)),
            dma((count,)),
        ],
        compiler_params=pltpu.CompilerParams(
            collective_id=0, has_side_effects=True, vmem_limit_bytes=40 * 1024 * 1024
        ),
    )(
        head,
        ks,
        classes,
        vg_alpha,
        vg_shape,
        bed,
        flow_code,
        surface_soil,
        cover_class,
        ponding,
        conveyance,
        erodibility,
    )
    return jnp.swapaxes(head_out, 0, 1), bed_out


def solution(mesh):
    in_specs = (
        P("member", "tile", None),
        P("member", "tile", None),
        P("member", "tile", None),
        P(),
        P(),
        P("tile", "member"),
        P("tile", "member"),
        P("tile", "member"),
        P("tile", "member"),
        P("tile", "member"),
        P(),
        P(),
    )
    out_specs = (P("member", "tile", None), P("tile", "member"))
    return jax.shard_map(
        on_device, mesh=mesh, in_specs=in_specs, out_specs=out_specs, check_vma=False
    )
```
